512 devices in a mesh: blk: 128 (over x_lo, y, z), grp: 4 (over x_hi, core).
Axes of the slice: x: 4 (x_hi: 2, x_lo: 2; x = x_hi * 2 + x_lo), y: 4, z: 16, core: 2. Of those that a mesh axis runs over, the one named last changes fastest.
Arguments:
- tables: float32 [8, 131072, 128], P('grp', 'blk'), may hold values from -1 to 1
- bag_ids: int32 [16384, 8, 32], P('blk', 'grp'), may hold values from 0 to 8191, as said below
Outputs:
- pooled: float32 [16384, 8, 128], P('blk', 'grp')
- interaction: float32 [16384, 8, 8], P('blk', 'grp')
The draws below stay inside these ranges and needn't reach their ends.
Inputs may be any that keep to these rules, and one draw needn't show every extreme that they name: `bag_ids`: some rows are far more popular than others.
All inputs are finite; a program needn't handle non-finite values.
Results may differ from the reference program's by a relative error of at most 0.000065.
Values sent between devices are 32-bit elements; how exact they have to be, the bound alone decides.
No kernel may reach another device: no remote copies, remote signals or barrier semaphores. Data moves between devices by JAX's collectives and lax.ppermute only.
A program may use at most 64 MiB of HBM per device.

```python
import math
import jax
import jax.numpy as jnp
from jax import lax

E = 128
ROWS_DEV = 1024
BAG = 32
SECTIONS = 8
B_DEV = 128
ROWS = 131072
TABLES = 8
BATCH = 16384
N_BLK = 128


def draw_bag_ids(key, part):
    subkeys = jax.random.split(key, 5)
    id_shape = (BATCH, TABLES, BAG)
    distance = jax.random.randint(subkeys[0], id_shape, 0, SECTIONS)
    uniform_rows = jax.random.randint(subkeys[1], id_shape, 0, ROWS_DEV)
    hot_table = jax.random.randint(subkeys[2], (TABLES, 16), 0, ROWS_DEV)
    hot_pick = jax.random.randint(subkeys[3], id_shape, 0, 16)
    hot_rows = hot_table[jnp.arange(TABLES, dtype=jnp.int32)[None, :, None], hot_pick]
    popular = jax.random.randint(subkeys[4], id_shape, 0, 3) == 0
    row_choice = jnp.where(popular, hot_rows, uniform_rows)
    return (row_choice * SECTIONS + distance).astype(jnp.int32)


def levels(own_key, shape, cuts, least, top_value):
    loudness, own = 1.0, jax.random.fold_in(own_key, 6)
    for axis_at, parts in cuts:
        heights = jnp.exp(jax.random.uniform(jax.random.fold_in(own, axis_at), (parts,), jnp.float32, least / len(cuts), top_value / len(cuts)))
        loudness = loudness * jnp.repeat(heights, shape[axis_at] // parts).reshape([-1 if axis == axis_at else 1 for axis in range(len(shape))])
    return loudness


def scatter_about(rng, shape, deviation, most, pieces=(), kind=jnp.bfloat16):
    gain = levels(rng, shape, pieces, -0.22, 0.18) if pieces else 1.0
    entries = jax.random.normal(rng, shape, jnp.float32) * deviation * gain
    return jnp.minimum(jnp.maximum(entries, -most), most).astype(kind)


def setup_inputs(seed: int = 0) -> dict:
    keys = jax.random.split(jax.random.key(seed), 3)
    return {
        "tables": scatter_about(keys[0], (TABLES, ROWS, E), 0.18, 1.0, ((0, 4), (1, 128)), jnp.float32),
        "bag_ids": draw_bag_ids(jax.random.fold_in(keys[2], 71), 0),
    }


def reference(tables, bag_ids):
    home_shard = (jnp.arange(BATCH, dtype=jnp.int32) // B_DEV)[:, None, None]
    distance = bag_ids % SECTIONS
    local_row = bag_ids // SECTIONS
    row_index = (((home_shard - distance) % N_BLK) * ROWS_DEV + local_row).astype(jnp.int32)
    block_size = math.gcd(BATCH, 512)
    grouped = row_index.reshape(BATCH // block_size, block_size, TABLES, BAG)

    def one_block(block_ids):
        columns = [jnp.sum(tables[table_num][block_ids[:, table_num, :]], axis=1) for table_num in range(TABLES)]
        return jnp.stack(columns, axis=1)

    pooled = lax.map(one_block, grouped).reshape(BATCH, TABLES, E)
    interaction = jnp.einsum("bte,bue->btu", pooled, pooled, precision=lax.Precision.HIGHEST) / E
    return pooled, interaction
```

```python
import jax
import jax.numpy as jnp
from jax import lax
from jax.experimental import pallas as pl
from jax.experimental.pallas import tpu as pltpu
from jax.sharding import PartitionSpec as P

SECTIONS = 8
VMEM_LIMIT = 8 * 1024 * 1024


def shift(value, axis, steps):
    count = lax.axis_size(axis)
    pairs = [(source, (source + steps) % count) for source in range(count)]
    return lax.ppermute(value, axis, pairs)


def vmem(count):
    return [pl.BlockSpec(memory_space=pltpu.VMEM)] * count


def prepare(tables):
    count, rows, width = tables.shape

    def kernel(table_ref, out_ref):
        for table_num in range(count):
            for start in range(0, rows, 256):
                part = table_ref[table_num, start : start + 256, :].T
                high = part.astype(jnp.bfloat16)
                low = (part - high.astype(jnp.float32)).astype(jnp.bfloat16)
                out_ref[table_num, :width, start : start + 256] = high
                out_ref[table_num, width:, start : start + 256] = low

    return pl.pallas_call(
        kernel,
        out_shape=jax.ShapeDtypeStruct((count, 2 * width, rows), jnp.bfloat16),
        in_specs=vmem(1),
        out_specs=vmem(1)[0],
        cost_estimate=pl.CostEstimate(flops=4_000_000, bytes_accessed=2_000_000, transcendentals=0),
        compiler_params=pltpu.CompilerParams(vmem_limit_bytes=VMEM_LIMIT),
        name="prepare",
    )(tables)


def add_counts(codes, offset, count_ref, slots, chunk):
    samples = codes.shape[1]
    row = lax.shift_right_logical(codes, 3)
    slot = row & (slots - 1)
    lane = lax.shift_right_logical(row, 8) * 8
    unit = jnp.where((codes & (SECTIONS - 1)) == offset, jnp.left_shift(1, lane), 0)
    for start in range(0, slots, chunk):
        place = lax.broadcasted_iota(jnp.int32, (chunk, samples), 0) + start
        total = jnp.zeros((chunk, samples), jnp.int32)
        for entry in range(codes.shape[0]):
            total = total + jnp.where(
                place == slot[entry : entry + 1, :], unit[entry : entry + 1, :], 0
            )
        for quarter in range(4):
            piece = lax.shift_right_logical(total, 8 * quarter) & 255
            at = quarter * slots + start
            count_ref[at : at + chunk, :] = piece.astype(jnp.float32).astype(jnp.bfloat16)


def visit(split, state, offset, fresh, keep):
    tables, twice, rows = split.shape
    width = twice // 2
    samples = state.shape[1]
    head = tables * width
    base = 0 if fresh else head
    entries = state.shape[0] - base
    bag = entries // tables

    def kernel(split_ref, state_ref, out_ref, count_ref):
        for table_num in range(tables):
            first = base + table_num * bag
            codes = state_ref[first : first + bag, :].astype(jnp.int32)
            add_counts(codes, offset, count_ref.at[table_num], rows // 4, 128)
            both = jnp.dot(
                split_ref[table_num], count_ref[table_num], preferred_element_type=jnp.float32
            )
            value = both[:width] + both[width:]
            at = table_num * width
            if not fresh:
                value = value + state_ref[at : at + width, :]
            out_ref[at : at + width, :] = value
        if keep:
            out_ref[head:, :] = state_ref[base:, :]

    return pl.pallas_call(
        kernel,
        out_shape=jax.ShapeDtypeStruct((head + (entries if keep else 0), samples), jnp.float32),
        in_specs=vmem(2),
        out_specs=vmem(1)[0],
        scratch_shapes=[pltpu.VMEM((tables, rows, samples), jnp.bfloat16)],
        cost_estimate=pl.CostEstimate(flops=140_000_000, bytes_accessed=1_300_000, transcendentals=0),
        compiler_params=pltpu.CompilerParams(vmem_limit_bytes=VMEM_LIMIT),
        name="visit%d" % offset,
    )(split, state)


def join(one, two, tables):
    height, samples = one.shape
    width = height // tables

    def kernel(one_ref, two_ref, sum_ref, out_ref):
        for table_num in range(tables):
            at = table_num * width
            value = one_ref[at : at + width, :] + two_ref[at : at + width, :]
            sum_ref[at : at + width, :] = value
            out_ref[:, table_num, :] = value.T

    return pl.pallas_call(
        kernel,
        out_shape=(
            jax.ShapeDtypeStruct((height, samples), jnp.float32),
            jax.ShapeDtypeStruct((samples, tables, width), jnp.float32),
        ),
        in_specs=vmem(2),
        out_specs=tuple(vmem(2)),
        cost_estimate=pl.CostEstimate(flops=4_000_000, bytes_accessed=500_000, transcendentals=0),
        compiler_params=pltpu.CompilerParams(vmem_limit_bytes=VMEM_LIMIT),
        name="join",
    )(one, two)


def interact(pooled, gathered, width):
    samples = pooled.shape[1]
    tables = pooled.shape[0] // width
    others = gathered.shape[0] // width

    def kernel(pooled_ref, gathered_ref, inter_ref):
        rows = []
        for table_num in range(tables):
            own = pooled_ref[table_num * width : (table_num + 1) * width, :]
            for other in range(others):
                there = gathered_ref[other * width : (other + 1) * width, :]
                rows.append(jnp.sum(own * there, axis=0, keepdims=True))
        inter_ref[...] = jnp.concatenate(rows, axis=0) / width

    return pl.pallas_call(
        kernel,
        out_shape=jax.ShapeDtypeStruct((tables * others, samples), jnp.float32),
        in_specs=vmem(2),
        out_specs=vmem(1)[0],
        cost_estimate=pl.CostEstimate(flops=4_000_000, bytes_accessed=700_000, transcendentals=0),
        compiler_params=pltpu.CompilerParams(vmem_limit_bytes=VMEM_LIMIT),
        name="interact",
    )(pooled, gathered)


def shards(tables, bag_ids):
    samples, count, bag = bag_ids.shape
    width = tables.shape[2]
    ids = bag_ids.reshape(samples, count * bag).T.astype(jnp.float32)
    far = shift(ids, "blk", -7)
    split = prepare(tables)
    back = visit(split, ids, 0, True, True)
    back = shift(back, "blk", -1)
    ahead = visit(split, far, 7, True, True)
    ahead = shift(ahead, "blk", 1)
    back = shift(visit(split, back, 1, False, True), "blk", -1)
    ahead = shift(visit(split, ahead, 6, False, True), "blk", 1)
    back = shift(visit(split, back, 2, False, True), "blk", -1)
    ahead = shift(visit(split, ahead, 5, False, True), "blk", 1)
    back = shift(visit(split, back, 3, False, False), "blk", -1)
    ahead = visit(split, ahead, 4, False, False)
    pooled, result = join(ahead, back, count)
    result = shift(result, "blk", 4)
    gathered = lax.all_gather(pooled, "grp", axis=0, tiled=True)
    inter = shift(interact(pooled, gathered, width), "blk", 4)
    return result, inter.reshape(count, -1, samples).transpose(2, 0, 1)


def solution(mesh):
    return jax.shard_map(
        shards,
        mesh=mesh,
        in_specs=(P("grp", "blk", None), P("blk", "grp", None)),
        out_specs=(P("blk", "grp", None), P("blk", "grp", None)),
        check_vma=False,
    )
```

```python
import jax
import jax.numpy as jnp
from jax import lax
from jax.experimental import pallas as pl
from jax.experimental.pallas import tpu as pltpu
from jax.sharding import PartitionSpec as P


SECTIONS = 8
VMEM_LIMIT = 8 * 1024 * 1024


def shift(value, axis, steps):
    count = lax.axis_size(axis)
    pairs = [(source, (source + steps) % count) for source in range(count)]
    return lax.ppermute(value, axis, pairs)


def vmem(count):
    return [pl.BlockSpec(memory_space=pltpu.VMEM)] * count


def prepare(tables):
    count, rows, width = tables.shape

    def kernel(table_ref, out_ref):
        for table_num in range(count):
            for start in range(0, rows, 256):
                part = table_ref[table_num, start : start + 256, :].T
                high = part.astype(jnp.bfloat16)
                low = (part - high.astype(jnp.float32)).astype(jnp.bfloat16)
                out_ref[table_num, :width, start : start + 256] = high
                out_ref[table_num, width:, start : start + 256] = low

    return pl.pallas_call(
        kernel,
        out_shape=jax.ShapeDtypeStruct((count, 2 * width, rows), jnp.bfloat16),
        in_specs=vmem(1),
        out_specs=vmem(1)[0],
        cost_estimate=pl.CostEstimate(flops=4_000_000, bytes_accessed=2_000_000, transcendentals=0),
        compiler_params=pltpu.CompilerParams(vmem_limit_bytes=VMEM_LIMIT),
        name="prepare",
    )(tables)


def add_counts(codes, offset, count_ref):
    rows, samples = count_ref.shape
    slots = rows // 8
    entries = codes.shape[0]
    row = lax.shift_right_logical(codes, 3)
    slot = row & (slots - 1)
    place4 = lax.shift_right_logical(row, slots.bit_length() - 1) * 4
    unit = jnp.where((codes & (SECTIONS - 1)) == offset, jnp.left_shift(1, place4), 0)
    mask = 0x0F0F0F0F
    for start in range(0, slots, 64):
        place = lax.broadcasted_iota(jnp.int32, (64, samples), 0) + start
        even = odd = None
        for first in range(0, entries, 11):
            total = jnp.zeros((64, samples), jnp.int32)
            for entry in range(first, min(first + 11, entries)):
                total = total + jnp.where(
                    place == slot[entry : entry + 1, :], unit[entry : entry + 1, :], 0
                )
            low = total & mask
            high = lax.shift_right_logical(total, 4) & mask
            even = low if even is None else even + low
            odd = high if odd is None else odd + high
        for pair in range(4):
            for half, word in enumerate((even, odd)):
                piece = lax.shift_right_logical(word, 8 * pair) & 255
                at = (2 * pair + half) * slots + start
                count_ref[at : at + 64, :] = piece.astype(jnp.float32).astype(jnp.bfloat16)


def visit(split, state, offset, fresh, keep):
    tables, twice, rows = split.shape
    width = twice // 2
    samples = state.shape[1]
    head = tables * width
    base = 0 if fresh else head
    entries = state.shape[0] - base
    bag = entries // tables

    def kernel(split_ref, state_ref, out_ref, count_ref):
        for table_num in range(tables):
            first = base + table_num * bag
            codes = state_ref[first : first + bag, :].astype(jnp.int32)
            add_counts(codes, offset, count_ref.at[table_num])
            both = jnp.dot(
                split_ref[table_num], count_ref[table_num], preferred_element_type=jnp.float32
            )
            value = both[:width] + both[width:]
            at = table_num * width
            if not fresh:
                value = value + state_ref[at : at + width, :]
            out_ref[at : at + width, :] = value
        if keep:
            out_ref[head:, :] = state_ref[base:, :].astype(jnp.float32)

    return pl.pallas_call(
        kernel,
        out_shape=jax.ShapeDtypeStruct((head + (entries if keep else 0), samples), jnp.float32),
        in_specs=vmem(2),
        out_specs=vmem(1)[0],
        scratch_shapes=[pltpu.VMEM((tables, rows, samples), jnp.bfloat16)],
        cost_estimate=pl.CostEstimate(flops=140_000_000, bytes_accessed=1_300_000, transcendentals=0),
        compiler_params=pltpu.CompilerParams(vmem_limit_bytes=VMEM_LIMIT),
    )(split, state)


def join(one, two, tables):
    height, samples = one.shape
    width = height // tables

    def kernel(one_ref, two_ref, sum_ref, out_ref):
        for table_num in range(tables):
            at = table_num * width
            value = one_ref[at : at + width, :] + two_ref[at : at + width, :]
            sum_ref[at : at + width, :] = value
            out_ref[:, table_num, :] = value.T

    return pl.pallas_call(
        kernel,
        out_shape=(
            jax.ShapeDtypeStruct((height, samples), jnp.float32),
            jax.ShapeDtypeStruct((samples, tables, width), jnp.float32),
        ),
        in_specs=vmem(2),
        out_specs=tuple(vmem(2)),
        cost_estimate=pl.CostEstimate(flops=4_000_000, bytes_accessed=500_000, transcendentals=0),
        compiler_params=pltpu.CompilerParams(vmem_limit_bytes=VMEM_LIMIT),
        name="join",
    )(one, two)


def interact(pooled, gathered, width):
    samples = pooled.shape[1]
    tables = pooled.shape[0] // width
    others = gathered.shape[0] // width

    def kernel(pooled_ref, gathered_ref, inter_ref):
        rows = []
        for table_num in range(tables):
            own = pooled_ref[table_num * width : (table_num + 1) * width, :]
            for other in range(others):
                there = gathered_ref[other * width : (other + 1) * width, :]
                rows.append(jnp.sum(own * there, axis=0, keepdims=True))
        inter_ref[...] = jnp.concatenate(rows, axis=0) / width

    return pl.pallas_call(
        kernel,
        out_shape=jax.ShapeDtypeStruct((tables * others, samples), jnp.float32),
        in_specs=vmem(2),
        out_specs=vmem(1)[0],
        cost_estimate=pl.CostEstimate(flops=4_000_000, bytes_accessed=700_000, transcendentals=0),
        compiler_params=pltpu.CompilerParams(vmem_limit_bytes=VMEM_LIMIT),
        name="interact",
    )(pooled, gathered)


def shards(tables, bag_ids):
    samples, count, bag = bag_ids.shape
    width = tables.shape[2]
    ids = bag_ids.reshape(samples, count * bag).T
    far = shift(ids, "blk", -7)
    split = prepare(tables)
    back = visit(split, ids, 0, True, True)
    back = shift(back, "blk", -1)
    ahead = visit(split, far, 7, True, True)
    ahead = shift(ahead, "blk", 1)
    back = shift(visit(split, back, 1, False, True), "blk", -1)
    ahead = shift(visit(split, ahead, 6, False, True), "blk", 1)
    back = shift(visit(split, back, 2, False, True), "blk", -1)
    ahead = shift(visit(split, ahead, 5, False, True), "blk", 1)
    back = shift(visit(split, back, 3, False, False), "blk", -1)
    ahead = visit(split, ahead, 4, False, False)
    pooled, result = join(ahead, back, count)
    result = shift(result, "blk", 4)
    gathered = lax.all_gather(pooled, "grp", axis=0, tiled=True)
    inter = interact(pooled, gathered, width)
    inter = shift(inter, "blk", 4)
    return result, inter.reshape(count, -1, samples).transpose(2, 0, 1)


def solution(mesh):
    return jax.shard_map(
        shards,
        mesh=mesh,
        in_specs=(P("grp", "blk", None), P("blk", "grp", None)),
        out_specs=(P("blk", "grp", None), P("blk", "grp", None)),
        check_vma=False,
    )
```

```python
import jax
import jax.numpy as jnp
from jax import lax
from jax.experimental import pallas as pl
from jax.experimental.pallas import tpu as pltpu
from jax.sharding import PartitionSpec as P


SECTIONS = 8
VMEM_LIMIT = 8 * 1024 * 1024


def shift(value, axis, steps):
    count = lax.axis_size(axis)
    pairs = [(source, (source + steps) % count) for source in range(count)]
    return lax.ppermute(value, axis, pairs)


def vmem(count):
    return [pl.BlockSpec(memory_space=pltpu.VMEM)] * count


def prepare(tables):
    count, rows, width = tables.shape

    def kernel(table_ref, out_ref):
        for table_num in range(count):
            for start in range(0, rows, 256):
                part = table_ref[table_num, start : start + 256, :].T
                high = part.astype(jnp.bfloat16)
                low = (part - high.astype(jnp.float32)).astype(jnp.bfloat16)
                out_ref[table_num, :width, start : start + 256] = high
                out_ref[table_num, width:, start : start + 256] = low

    return pl.pallas_call(
        kernel,
        out_shape=jax.ShapeDtypeStruct((count, 2 * width, rows), jnp.bfloat16),
        in_specs=vmem(1),
        out_specs=vmem(1)[0],
        cost_estimate=pl.CostEstimate(flops=4_000_000, bytes_accessed=2_000_000, transcendentals=0),
        compiler_params=pltpu.CompilerParams(vmem_limit_bytes=VMEM_LIMIT),
        name="prepare",
    )(tables)


def count_rows(codes, offset, first_row, height):
    samples = codes.shape[1]
    entries = codes.shape[0]
    slots = height // 16
    row = lax.shift_right_logical(codes, 3) - first_row
    hit = ((codes & (SECTIONS - 1)) == offset) & (row >= 0) & (row < height)
    slot = jnp.where(hit, row & (slots - 1), -1)
    unit = jnp.left_shift(1, lax.shift_right_logical(row, slots.bit_length() - 1) * 2 & 31)
    place = lax.broadcasted_iota(jnp.int32, (slots, samples), 0)

    def plus(total, more):
        return more if total is None else [x + y for x, y in zip(total, more)]

    def split(word, bits, mask):
        return [word & mask, lax.shift_right_logical(word, bits) & mask]

    eight = None
    for first in range(0, entries, 15):
        four = None
        for start in range(first, min(first + 15, entries), 3):
            two = None
            for entry in range(start, min(start + 3, entries)):
                one = jnp.where(
                    place == slot[entry : entry + 1, :], unit[entry : entry + 1, :], 0
                )
                two = one if two is None else two + one
            four = plus(four, split(two, 2, 0x33333333))
        more = [piece for word in four for piece in split(word, 4, 0x0F0F0F0F)]
        eight = plus(eight, more)
    pieces = []
    for quarter in range(4):
        for word in (eight[0], eight[2], eight[1], eight[3]):
            piece = lax.shift_right_logical(word, 8 * quarter)
            if quarter < 3:
                piece = piece & 255
            pieces.append(piece.astype(jnp.float32).astype(jnp.bfloat16))
    return jnp.concatenate(pieces, axis=0)


def add_rows(split_ref, table_num, codes, offset):
    width = split_ref.shape[1] // 2
    rows = split_ref.shape[2]
    half = 512
    value = None
    for first in range(0, rows, half):
        counts = count_rows(codes, offset, first, half)
        for part in range(2):
            product = jnp.dot(
                split_ref[table_num, part * width : (part + 1) * width, first : first + half],
                counts,
                preferred_element_type=jnp.float32,
            )
            value = product if value is None else value + product
    return value


def visit(split, state, offset, fresh, keep):
    tables, twice, _ = split.shape
    width = twice // 2
    samples = state.shape[1]
    head = tables * width
    base = 0 if fresh else head
    entries = state.shape[0] - base
    bag = entries // tables

    def kernel(split_ref, state_ref, out_ref):
        for table_num in range(tables):
            first = base + table_num * bag
            codes = state_ref[first : first + bag, :].astype(jnp.int32)
            value = add_rows(split_ref, table_num, codes, offset)
            at = table_num * width
            if not fresh:
                value = value + state_ref[at : at + width, :]
            out_ref[at : at + width, :] = value
        if keep:
            out_ref[head:, :] = state_ref[base:, :].astype(jnp.float32)

    return pl.pallas_call(
        kernel,
        out_shape=jax.ShapeDtypeStruct((head + (entries if keep else 0), samples), jnp.float32),
        in_specs=vmem(2),
        out_specs=vmem(1)[0],
        cost_estimate=pl.CostEstimate(flops=140_000_000, bytes_accessed=1_300_000, transcendentals=0),
        compiler_params=pltpu.CompilerParams(vmem_limit_bytes=VMEM_LIMIT),
    )(split, state)


def deliver(pooled, tables):
    height, samples = pooled.shape
    width = height // tables

    def kernel(pooled_ref, out_ref):
        for table_num in range(tables):
            at = table_num * width
            out_ref[:, table_num, :] = pooled_ref[at : at + width, :].T

    return pl.pallas_call(
        kernel,
        out_shape=jax.ShapeDtypeStruct((samples, tables, width), jnp.float32),
        in_specs=vmem(1),
        out_specs=vmem(1)[0],
        cost_estimate=pl.CostEstimate(flops=1_000_000, bytes_accessed=300_000, transcendentals=0),
        compiler_params=pltpu.CompilerParams(vmem_limit_bytes=VMEM_LIMIT),
        name="deliver",
    )(pooled)


def interact(pooled, gathered, width):
    samples = pooled.shape[1]
    tables = pooled.shape[0] // width
    others = gathered.shape[0] // width

    def kernel(pooled_ref, gathered_ref, inter_ref):
        rows = []
        for table_num in range(tables):
            own = pooled_ref[table_num * width : (table_num + 1) * width, :]
            for other in range(others):
                there = gathered_ref[other * width : (other + 1) * width, :]
                rows.append(jnp.sum(own * there, axis=0, keepdims=True))
        inter_ref[...] = jnp.concatenate(rows, axis=0) / width

    return pl.pallas_call(
        kernel,
        out_shape=jax.ShapeDtypeStruct((tables * others, samples), jnp.float32),
        in_specs=vmem(2),
        out_specs=vmem(1)[0],
        cost_estimate=pl.CostEstimate(flops=4_000_000, bytes_accessed=700_000, transcendentals=0),
        compiler_params=pltpu.CompilerParams(vmem_limit_bytes=VMEM_LIMIT),
        name="interact",
    )(pooled, gathered)


def shards(tables, bag_ids):
    samples, count, bag = bag_ids.shape
    width = tables.shape[2]
    ids = bag_ids.reshape(samples, count * bag).T
    far = shift(ids, "blk", -7)
    split = prepare(tables)
    back = visit(split, ids, 0, True, True)
    back = shift(back, "blk", -1)
    ahead = visit(split, far, 7, True, True)
    ahead = shift(ahead, "blk", 1)
    back = shift(visit(split, back, 1, False, True), "blk", -1)
    ahead = shift(visit(split, ahead, 6, False, True), "blk", 1)
    back = shift(visit(split, back, 2, False, True), "blk", -1)
    ahead = shift(visit(split, ahead, 5, False, True), "blk", 1)
    back = shift(visit(split, back, 3, False, False), "blk", -1)
    ahead = visit(split, ahead, 4, False, False)
    pooled = ahead + back
    result = shift(pooled, "blk", 4)
    gathered = lax.all_gather(pooled, "grp", axis=0, tiled=True)
    inter = interact(pooled, gathered, width)
    inter = shift(inter, "blk", 4)
    result = deliver(result, count)
    return result, inter.reshape(count, -1, samples).transpose(2, 0, 1)


def solution(mesh):
    return jax.shard_map(
        shards,
        mesh=mesh,
        in_specs=(P("grp", "blk", None), P("blk", "grp", None)),
        out_specs=(P("blk", "grp", None), P("blk", "grp", None)),
        check_vma=False,
    )
```

```python
import jax
import jax.numpy as jnp
from jax import lax
from jax.experimental import pallas as pl
from jax.experimental.pallas import tpu as pltpu
from jax.sharding import PartitionSpec as P


SECTIONS = 8
VMEM_LIMIT = 8 * 1024 * 1024


def shift(value, axis, steps):
    count = lax.axis_size(axis)
    pairs = [(source, (source + steps) % count) for source in range(count)]
    return lax.ppermute(value, axis, pairs)


def vmem(count):
    return [pl.BlockSpec(memory_space=pltpu.VMEM)] * count


def prepare(tables):
    count, rows, width = tables.shape

    def kernel(table_ref, out_ref):
        for table_num in range(count):
            for start in range(0, rows, 256):
                part = table_ref[table_num, start : start + 256, :].T
                high = part.astype(jnp.bfloat16)
                low = (part - high.astype(jnp.float32)).astype(jnp.bfloat16)
                out_ref[table_num, :width, start : start + 256] = high
                out_ref[table_num, width:, start : start + 256] = low

    return pl.pallas_call(
        kernel,
        out_shape=jax.ShapeDtypeStruct((count, 2 * width, rows), jnp.bfloat16),
        in_specs=vmem(1),
        out_specs=vmem(1)[0],
        cost_estimate=pl.CostEstimate(flops=4_000_000, bytes_accessed=2_000_000, transcendentals=0),
        compiler_params=pltpu.CompilerParams(vmem_limit_bytes=VMEM_LIMIT),
        name="prepare",
    )(tables)


def place_ids(codes, offset, slot_ref, unit_ref):
    row = lax.shift_right_logical(codes, 3)
    slot = (row & 31) | (lax.shift_right_logical(row, 9) << 5)
    slot_ref[...] = jnp.where((codes & (SECTIONS - 1)) == offset, slot, -1)
    unit_ref[...] = jnp.left_shift(1, (lax.shift_right_logical(row, 5) & 15) * 2)


def count_rows(slot_ref, unit_ref, first, entries, chunk):
    samples = slot_ref.shape[1]
    place = lax.broadcasted_iota(jnp.int32, (32, samples), 0) + 32 * chunk

    def row_of(ref, entry):
        return jnp.broadcast_to(ref[first + entry : first + entry + 1, :], (32, samples))

    def plus(total, more):
        return more if total is None else [x + y for x, y in zip(total, more)]

    def split(word, bits, mask):
        return [word & mask, lax.shift_right_logical(word, bits) & mask]

    eight = None
    for block in range(0, entries, 15):
        four = None
        for start in range(block, min(block + 15, entries), 3):
            two = None
            for entry in range(start, min(start + 3, entries)):
                one = jnp.where(
                    place == row_of(slot_ref, entry), row_of(unit_ref, entry), 0
                )
                two = one if two is None else two + one
            four = plus(four, split(two, 2, 0x33333333))
        more = [piece for word in four for piece in split(word, 4, 0x0F0F0F0F)]
        eight = plus(eight, more)
    pieces = []
    for quarter in range(4):
        for word in (eight[0], eight[2], eight[1], eight[3]):
            piece = lax.shift_right_logical(word, 8 * quarter)
            if quarter < 3:
                piece = piece & 255
            pieces.append(piece.astype(jnp.float32).astype(jnp.bfloat16))
    return jnp.concatenate(pieces, axis=0)


def add_rows(split_ref, table_num, slot_ref, unit_ref, bag):
    width = split_ref.shape[1] // 2
    rows = split_ref.shape[2]
    value = None
    for chunk in range(rows // 512):
        counts = count_rows(slot_ref, unit_ref, table_num * bag, bag, chunk)
        both = jnp.dot(
            split_ref[table_num, :, chunk * 512 : (chunk + 1) * 512],
            counts,
            preferred_element_type=jnp.float32,
        )
        value = both if value is None else value + both
    return value[:width] + value[width:]


def visit(split, state, offset, fresh, keep):
    tables, twice, _ = split.shape
    width = twice // 2
    samples = state.shape[1]
    head = tables * width
    base = 0 if fresh else head
    entries = state.shape[0] - base
    bag = entries // tables

    def kernel(split_ref, state_ref, out_ref, slot_ref, unit_ref):
        place_ids(state_ref[base:, :].astype(jnp.int32), offset, slot_ref, unit_ref)
        for table_num in range(tables):
            value = add_rows(split_ref, table_num, slot_ref, unit_ref, bag)
            at = table_num * width
            if not fresh:
                value = value + state_ref[at : at + width, :]
            out_ref[at : at + width, :] = value
        if keep:
            out_ref[head:, :] = state_ref[base:, :].astype(jnp.float32)

    return pl.pallas_call(
        kernel,
        out_shape=jax.ShapeDtypeStruct((head + (entries if keep else 0), samples), jnp.float32),
        in_specs=vmem(2),
        out_specs=vmem(1)[0],
        scratch_shapes=[pltpu.VMEM((entries, samples), jnp.int32)] * 2,
        cost_estimate=pl.CostEstimate(flops=140_000_000, bytes_accessed=1_300_000, transcendentals=0),
        compiler_params=pltpu.CompilerParams(vmem_limit_bytes=VMEM_LIMIT),
    )(split, state)


def deliver(pooled, tables):
    height, samples = pooled.shape
    width = height // tables

    def kernel(pooled_ref, out_ref):
        for table_num in range(tables):
            at = table_num * width
            out_ref[:, table_num, :] = pooled_ref[at : at + width, :].T

    return pl.pallas_call(
        kernel,
        out_shape=jax.ShapeDtypeStruct((samples, tables, width), jnp.float32),
        in_specs=vmem(1),
        out_specs=vmem(1)[0],
        cost_estimate=pl.CostEstimate(flops=1_000_000, bytes_accessed=300_000, transcendentals=0),
        compiler_params=pltpu.CompilerParams(vmem_limit_bytes=VMEM_LIMIT),
        name="deliver",
    )(pooled)


def interact(pooled, gathered, width):
    samples = pooled.shape[1]
    tables = pooled.shape[0] // width
    others = gathered.shape[0] // width

    def kernel(pooled_ref, gathered_ref, inter_ref):
        rows = []
        for table_num in range(tables):
            own = pooled_ref[table_num * width : (table_num + 1) * width, :]
            for other in range(others):
                there = gathered_ref[other * width : (other + 1) * width, :]
                rows.append(jnp.sum(own * there, axis=0, keepdims=True))
        inter_ref[...] = jnp.concatenate(rows, axis=0) / width

    return pl.pallas_call(
        kernel,
        out_shape=jax.ShapeDtypeStruct((tables * others, samples), jnp.float32),
        in_specs=vmem(2),
        out_specs=vmem(1)[0],
        cost_estimate=pl.CostEstimate(flops=4_000_000, bytes_accessed=700_000, transcendentals=0),
        compiler_params=pltpu.CompilerParams(vmem_limit_bytes=VMEM_LIMIT),
        name="interact",
    )(pooled, gathered)


def shards(tables, bag_ids):
    samples, count, bag = bag_ids.shape
    width = tables.shape[2]
    ids = bag_ids.reshape(samples, count * bag).T
    far = shift(ids, "blk", -7)
    split = prepare(tables)
    back = visit(split, ids, 0, True, True)
    back = shift(back, "blk", -1)
    ahead = visit(split, far, 7, True, True)
    ahead = shift(ahead, "blk", 1)
    back = shift(visit(split, back, 1, False, True), "blk", -1)
    ahead = shift(visit(split, ahead, 6, False, True), "blk", 1)
    back = shift(visit(split, back, 2, False, True), "blk", -1)
    ahead = shift(visit(split, ahead, 5, False, True), "blk", 1)
    back = shift(visit(split, back, 3, False, False), "blk", -1)
    ahead = visit(split, ahead, 4, False, False)
    pooled = ahead + back
    result = shift(pooled, "blk", 4)
    gathered = lax.all_gather(pooled, "grp", axis=0, tiled=True)
    inter = interact(pooled, gathered, width)
    inter = shift(inter, "blk", 4)
    result = deliver(result, count)
    return result, inter.reshape(count, -1, samples).transpose(2, 0, 1)


def solution(mesh):
    return jax.shard_map(
        shards,
        mesh=mesh,
        in_specs=(P("grp", "blk", None), P("blk", "grp", None)),
        out_specs=(P("blk", "grp", None), P("blk", "grp", None)),
        check_vma=False,
    )
```

```python
import jax
import jax.numpy as jnp
from jax import lax
from jax.experimental import pallas as pl
from jax.experimental.pallas import tpu as pltpu
from jax.sharding import PartitionSpec as P


SECTIONS = 8
VMEM_LIMIT = 8 * 1024 * 1024


def shift(value, axis, steps):
    count = lax.axis_size(axis)
    pairs = [(source, (source + steps) % count) for source in range(count)]
    return lax.ppermute(value, axis, pairs)


def vmem(count):
    return [pl.BlockSpec(memory_space=pltpu.VMEM)] * count


def prepare(tables):
    count, rows, width = tables.shape

    def kernel(table_ref, out_ref):
        for table_num in range(count):
            for start in range(0, rows, 256):
                part = table_ref[table_num, start : start + 256, :].T
                high = part.astype(jnp.bfloat16)
                low = (part - high.astype(jnp.float32)).astype(jnp.bfloat16)
                out_ref[table_num, :width, start : start + 256] = high
                out_ref[table_num, width:, start : start + 256] = low

    return pl.pallas_call(
        kernel,
        out_shape=jax.ShapeDtypeStruct((count, 2 * width, rows), jnp.bfloat16),
        in_specs=vmem(1),
        out_specs=vmem(1)[0],
        cost_estimate=pl.CostEstimate(flops=4_000_000, bytes_accessed=2_000_000, transcendentals=0),
        compiler_params=pltpu.CompilerParams(vmem_limit_bytes=VMEM_LIMIT),
        name="prepare",
    )(tables)


def place_ids(codes, offset, slot_ref, unit_ref):
    row = lax.shift_right_logical(codes, 3)
    slot = (row & 31) | (lax.shift_right_logical(row, 9) << 5)
    slot_ref[...] = jnp.where((codes & (SECTIONS - 1)) == offset, slot, -1)
    unit_ref[...] = jnp.left_shift(1, (lax.shift_right_logical(row, 5) & 15) * 2)


def count_rows(slot_ref, unit_ref, first, entries, chunk):
    samples = slot_ref.shape[1]
    place = lax.broadcasted_iota(jnp.int32, (32, samples), 0) + 32 * chunk

    def row_of(ref, entry):
        return jnp.broadcast_to(ref[first + entry : first + entry + 1, :], (32, samples))

    def plus(total, more):
        return more if total is None else [x + y for x, y in zip(total, more)]

    def split(word, bits, mask):
        return [word & mask, lax.shift_right_logical(word, bits) & mask]

    eight = None
    for block in range(0, entries, 15):
        four = None
        for start in range(block, min(block + 15, entries), 3):
            two = None
            for entry in range(start, min(start + 3, entries)):
                one = jnp.where(
                    place == row_of(slot_ref, entry), row_of(unit_ref, entry), 0
                )
                two = one if two is None else two + one
            four = plus(four, split(two, 2, 0x33333333))
        more = [piece for word in four for piece in split(word, 4, 0x0F0F0F0F)]
        eight = plus(eight, more)
    pieces = []
    for quarter in range(4):
        for word in (eight[0], eight[2], eight[1], eight[3]):
            piece = lax.shift_right_logical(word, 8 * quarter)
            if quarter < 3:
                piece = piece & 255
            pieces.append(piece.astype(jnp.float32).astype(jnp.bfloat16))
    return jnp.concatenate(pieces, axis=0)


def add_rows(split_ref, table_num, slot_ref, unit_ref, bag):
    width = split_ref.shape[1] // 2
    rows = split_ref.shape[2]
    value = None
    for chunk in range(rows // 512):
        counts = count_rows(slot_ref, unit_ref, table_num * bag, bag, chunk)
        both = jnp.dot(
            split_ref[table_num, :, chunk * 512 : (chunk + 1) * 512],
            counts,
            preferred_element_type=jnp.float32,
        )
        value = both if value is None else value + both
    return value[:width] + value[width:]


def visit(split, state, offset, fresh, keep):
    tables, twice, _ = split.shape
    width = twice // 2
    samples = state.shape[1]
    head = tables * width
    base = 0 if fresh else head
    entries = state.shape[0] - base
    bag = entries // tables

    def kernel(split_ref, state_ref, out_ref, slot_ref, unit_ref):
        place_ids(state_ref[base:, :].astype(jnp.int32), offset, slot_ref, unit_ref)
        for table_num in range(tables):
            value = add_rows(split_ref, table_num, slot_ref, unit_ref, bag)
            at = table_num * width
            if not fresh:
                value = value + state_ref[at : at + width, :]
            out_ref[at : at + width, :] = value
        if keep:
            out_ref[head:, :] = state_ref[base:, :].astype(jnp.float32)

    return pl.pallas_call(
        kernel,
        out_shape=jax.ShapeDtypeStruct((head + (entries if keep else 0), samples), jnp.float32),
        in_specs=vmem(2),
        out_specs=vmem(1)[0],
        scratch_shapes=[pltpu.VMEM((entries, samples), jnp.int32)] * 2,
        cost_estimate=pl.CostEstimate(flops=140_000_000, bytes_accessed=1_300_000, transcendentals=0),
        compiler_params=pltpu.CompilerParams(vmem_limit_bytes=VMEM_LIMIT),
    )(split, state)


def deliver(pooled, tables):
    height, samples = pooled.shape
    width = height // tables

    def kernel(pooled_ref, out_ref):
        for table_num in range(tables):
            at = table_num * width
            out_ref[:, table_num, :] = pooled_ref[at : at + width, :].T

    return pl.pallas_call(
        kernel,
        out_shape=jax.ShapeDtypeStruct((samples, tables, width), jnp.float32),
        in_specs=vmem(1),
        out_specs=vmem(1)[0],
        cost_estimate=pl.CostEstimate(flops=1_000_000, bytes_accessed=300_000, transcendentals=0),
        compiler_params=pltpu.CompilerParams(vmem_limit_bytes=VMEM_LIMIT),
        name="deliver",
    )(pooled)


def interact(parts, order, width):
    samples = parts[0].shape[1]
    tables = parts[0].shape[0] // width

    def kernel(order_ref, own_ref, all_ref, inter_ref):
        rows = {}
        for table_num in range(tables):
            own = own_ref[table_num * width : (table_num + 1) * width, :]
            for core in range(2):
                for place in range(2):
                    for one in range(tables):
                        at = ((core * 2 + place) * tables + one) * width
                        there = all_ref[at : at + width, :]
                        rows[table_num, place, core * tables + one] = jnp.sum(
                            own * there, axis=0, keepdims=True
                        )

        def stacked(first, second):
            pieces = []
            for table_num in range(tables):
                for place in (first, second):
                    for other in range(2 * tables):
                        pieces.append(rows[table_num, place, other])
            return jnp.concatenate(pieces, axis=0) / width

        inter_ref[...] = jnp.where(order_ref[0] == 0, stacked(0, 1), stacked(1, 0))

    return pl.pallas_call(
        kernel,
        out_shape=jax.ShapeDtypeStruct((tables * 4 * tables, samples), jnp.float32),
        in_specs=[pl.BlockSpec(memory_space=pltpu.SMEM)] + vmem(2),
        out_specs=vmem(1)[0],
        cost_estimate=pl.CostEstimate(flops=4_000_000, bytes_accessed=700_000, transcendentals=0),
        compiler_params=pltpu.CompilerParams(vmem_limit_bytes=VMEM_LIMIT),
        name="interact",
    )(order, *parts)


def shards(tables, bag_ids):
    samples, count, bag = bag_ids.shape
    width = tables.shape[2]
    ids = bag_ids.reshape(samples, count * bag).T
    far = shift(ids, "blk", -7)
    split = prepare(tables)
    back = visit(split, ids, 0, True, True)
    back = shift(back, "blk", -1)
    ahead = visit(split, far, 7, True, True)
    ahead = shift(ahead, "blk", 1)
    back = shift(visit(split, back, 1, False, True), "blk", -1)
    ahead = shift(visit(split, ahead, 6, False, True), "blk", 1)
    back = shift(visit(split, back, 2, False, True), "blk", -1)
    ahead = shift(visit(split, ahead, 5, False, True), "blk", 1)
    back = shift(visit(split, back, 3, False, False), "blk", -1)
    ahead = visit(split, ahead, 4, False, False)
    pooled = ahead + back
    result = shift(pooled, "blk", 4)
    cross = shift(pooled, "grp", 2)
    both = jnp.concatenate([pooled, cross], axis=0)
    gathered = lax.all_gather(both, "grp", axis=0, tiled=True, axis_index_groups=[[0, 1], [2, 3]])
    order = lax.axis_index("grp")[None] // 2
    inter = interact((pooled, gathered), order, width)
    inter = shift(inter, "blk", 4)
    result = deliver(result, count)
    return result, inter.reshape(count, -1, samples).transpose(2, 0, 1)


def solution(mesh):
    return jax.shard_map(
        shards,
        mesh=mesh,
        in_specs=(P("grp", "blk", None), P("blk", "grp", None)),
        out_specs=(P("blk", "grp", None), P("blk", "grp", None)),
        check_vma=False,
    )
```
